256 devices in a mesh: dp: 4 (over y), tensor: 64 (over x, z, core).
Axes of the slice: x: 4, y: 4, z: 8, core: 2. Of those that a mesh axis runs over, the one named last changes fastest.
Arguments:
- hidden_acts: bfloat16 [3, 1792, 14336], P(None, 'dp', 'tensor'), may hold values from -6 to 6
- out_grads: bfloat16 [3, 1792, 4096], P(None, 'dp', 'tensor'), may hold values from -6 to 6
Outputs:
- fisher: float32 [14336, 4096], P('tensor', 'dp')
The draws below stay inside these ranges and needn't reach their ends.
All inputs are finite; a program needn't handle non-finite values.
Results may differ from the reference program's by a relative error of at most 0.018.
Values may be sent and summed in bfloat16 or wider, within the bound.
No kernel may reach another device: no remote copies, remote signals or barrier semaphores. Data moves between devices by JAX's collectives and lax.ppermute only.
A program may use at most 64 MiB of HBM per device.

```python
import math
import jax
import jax.numpy as jnp
import numpy as np
from jax import lax

D = 4096
FF = 14336
FACTOR_A = 28
SEQS = 3
TOK_DEV = 448
SEQ_LEN = 1792
N_DP = 4


def level_of(own_key, dims, pieces, smallest, high):
    level = 1.0
    for axis_at, parts in pieces:
        draws = jax.random.uniform(jax.random.fold_in(jax.random.fold_in(own_key, 6), axis_at), (parts,), jnp.float32, smallest / len(pieces), high / len(pieces))
        level = level * jnp.repeat(jnp.exp(draws), dims[axis_at] // parts).reshape((-1,) + (1,) * (len(dims) - 1 - axis_at))
    return level


def gaussian(stream_key, shape, deviation, reach, cuts=(), kind=jnp.bfloat16):
    drawn = deviation * jax.random.normal(stream_key, shape, jnp.float32)
    if cuts:
        drawn = drawn * level_of(stream_key, shape, cuts, -0.22, 0.18)
    return jnp.clip(drawn, -reach, reach).astype(kind)


def setup_inputs(seed: int = 0) -> dict:
    arg_keys = jax.random.split(jax.random.key(seed), 3)
    return {
        "hidden_acts": gaussian(arg_keys[0], (SEQS, SEQ_LEN, FF), 1.0, 6.0, ((1, 4), (2, 64))),
        "out_grads": gaussian(arg_keys[1], (SEQS, SEQ_LEN, D), 1.0, 6.0, ((1, 4), (2, 64))),
    }


def sylvester(order):
    result = np.ones((1, 1))
    for doubling in range(order.bit_length() - 1):
        result = np.kron(result, np.array([[1.0, 1.0], [1.0, -1.0]]))
    return result

def paley_matrix():
    residues = set((number * number % 13 for number in range(1, 13)))
    core_table = np.zeros((14, 14))
    core_table[0, 1:] = 1.0
    core_table[1:, 0] = 1.0
    for row_index in range(13):
        for col_index in range(13):
            offset = (col_index - row_index) % 13
            if offset != 0:
                core_table[1 + row_index, 1 + col_index] = 1.0 if offset in residues else -1.0
    return np.kron(core_table, np.array([[1.0, 1.0], [1.0, -1.0]])) + np.kron(np.eye(14), np.array([[1.0, -1.0], [-1.0, -1.0]]))

def reference(hidden_acts, out_grads):
    factor_b = FF // FACTOR_A
    sylvester_table = jnp.asarray(sylvester(factor_b), jnp.float32)
    paley_table = jnp.asarray(paley_matrix(), jnp.float32)
    scaling = 1.0 / math.sqrt(FF)
    inv_root = 1.0 / math.sqrt(SEQ_LEN)
    highest = lax.Precision.HIGHEST
    fisher = jnp.zeros((FF, D), jnp.float32)
    for seq_index in range(SEQS):
        values = hidden_acts[seq_index].astype(jnp.float32).reshape(SEQ_LEN, factor_b, FACTOR_A)
        values = jnp.einsum('lba,bc->lca', values, sylvester_table, precision=highest)
        values = jnp.einsum('lca,ad->lcd', values, paley_table, precision=highest)
        rotated = (values.reshape(SEQ_LEN, FF) * scaling).astype(jnp.bfloat16)
        running = jnp.zeros((FF, D), jnp.float32)
        for block_idx in range(N_DP):
            token_rows = rotated[block_idx * TOK_DEV:(block_idx + 1) * TOK_DEV].astype(jnp.float32)
            grad_rows = out_grads[seq_index, block_idx * TOK_DEV:(block_idx + 1) * TOK_DEV].astype(jnp.float32)
            partial_sum = jnp.dot(token_rows.T, grad_rows, precision=highest)
            rounded = lax.optimization_barrier(partial_sum.astype(jnp.bfloat16))
            running = running + rounded.astype(jnp.float32)
        gradient = running * inv_root
        fisher = fisher + gradient * gradient
    return fisher / SEQS
```

```python
import math

import jax
import jax.numpy as jnp
import numpy as np
from jax import lax
from jax.experimental import pallas as pl
from jax.experimental.pallas import tpu as pltpu
from jax.sharding import PartitionSpec as P


FF = 14336
FACTOR_A = 28
SEQS = 3
X, Z, C, Y = 4, 8, 2, 4
LANES = 128
MIXED = X * Z
SHARE = 80


def sylvester(order):
    result = np.ones((1, 1))
    for _ in range(order.bit_length() - 1):
        result = np.kron(result, np.array([[1.0, 1.0], [1.0, -1.0]]))
    return result


def paley_matrix():
    residues = set((number * number % 13 for number in range(1, 13)))
    core_table = np.zeros((14, 14))
    core_table[0, 1:] = 1.0
    core_table[1:, 0] = 1.0
    for row_index in range(13):
        for col_index in range(13):
            offset = (col_index - row_index) % 13
            if offset != 0:
                core_table[1 + row_index, 1 + col_index] = 1.0 if offset in residues else -1.0
    return np.kron(core_table, np.array([[1.0, 1.0], [1.0, -1.0]])) + np.kron(
        np.eye(14), np.array([[1.0, -1.0], [-1.0, -1.0]])
    )


def place(x, z, c):
    return (x % X) * Z * C + (z % Z) * C + c


def pairs_of(target):
    return [
        (place(x, z, c), place(*target(x, z, c)))
        for x in range(X)
        for z in range(Z)
        for c in range(C)
    ]


CORE_SWAP = pairs_of(lambda x, z, c: (x, z, 1 - c))
X_UP = pairs_of(lambda x, z, c: (x + 1, z, c))
X_DOWN = pairs_of(lambda x, z, c: (x - 1, z, c))
Z_UP = pairs_of(lambda x, z, c: (x, z + 1, c))
Z_DOWN = pairs_of(lambda x, z, c: (x, z - 1, c))
Z_UP2 = pairs_of(lambda x, z, c: (x, z + 2, c))
Z_DOWN2 = pairs_of(lambda x, z, c: (x, z - 2, c))
Y_UP = [(y, (y + 1) % Y) for y in range(Y)]
Y_DOWN = [(y, (y - 1) % Y) for y in range(Y)]
XY_SWAP = [
    (y * X * Z * C + place(x, z, c), x * X * Z * C + place(y, z, c))
    for y in range(Y)
    for x in range(X)
    for z in range(Z)
    for c in range(C)
]
XZ_GROUPS = [[place(x, z, c) for x in range(X) for z in range(Z)] for c in range(C)]
PARCELS = ((0, -1, 1), (-2, -3, 2, 3), (4,))
FAR_CUTS = (1, 2, 1)
VMEM = pl.BlockSpec(memory_space=pltpu.VMEM)
SMEM = pl.BlockSpec(memory_space=pltpu.SMEM)


def call(kernel, out_shape, in_specs, flops, limit_mib, scratch=()):
    many = isinstance(out_shape, tuple)
    return pl.pallas_call(
        kernel,
        out_shape=out_shape,
        in_specs=in_specs,
        out_specs=(VMEM,) * len(out_shape) if many else VMEM,
        scratch_shapes=list(scratch),
        cost_estimate=pl.CostEstimate(flops=flops, bytes_accessed=2**20, transcendentals=0),
        compiler_params=pltpu.CompilerParams(vmem_limit_bytes=limit_mib * 2**20),
    )


def chip_rotation_kernel(place_ref, acts_ref, got_ref, rot_ref, out_ref):
    core = place_ref[0]
    half = got_ref.shape[1]
    rows = 7 * half // 2
    start = pl.multiple_of(core * half, half)
    for s in range(SEQS):
        inner = jnp.dot(
            acts_ref[s, pl.ds(start, half), :], rot_ref[core], preferred_element_type=jnp.float32
        ) + jnp.dot(got_ref[s], rot_ref[1 - core], preferred_element_type=jnp.float32)
        inner = inner.astype(jnp.bfloat16)
        for j in range(3):
            out_ref[rows * s + half * j : rows * s + half * (j + 1), :] = inner[
                :, LANES * j : LANES * (j + 1)
            ]
        out_ref[rows * s + half * 3 : rows * (s + 1), :] = jnp.concatenate(
            [inner[: half // 2, 3 * LANES :], inner[half // 2 :, 3 * LANES :]], axis=1
        )
    out_ref[rows * SEQS :, :] = jnp.zeros((MIXED * SHARE - rows * SEQS, LANES), jnp.bfloat16)


def butterfly(values):
    values = list(values)
    step = 1
    while step < len(values):
        for low in range(len(values)):
            if not low & step:
                a, b = values[low], values[low | step]
                values[low], values[low | step] = a + b, a - b
        step *= 2
    return values


def mix_kernel(scale, in_ref, out_ref, mid_ref):
    for r in range(0, SHARE, 16):
        rows = slice(r, r + 16)
        for x in range(X):
            mixed = butterfly([in_ref[x * Z + z, rows, :].astype(jnp.float32) for z in range(Z)])
            for z in range(Z):
                mid_ref[x * Z + z] = mixed[z]
        for z in range(Z):
            mixed = butterfly([mid_ref[x * Z + z] for x in range(X)])
            for x in range(X):
                out_ref[x * Z + z, rows, :] = (mixed[x] * scale).astype(jnp.bfloat16)


def partial_kernel(place_ref, r0, r1, r2a, r2b, r3, *refs):
    refs, (own_ref, other_ref, lhs_ref) = list(refs[:-3]), refs[-3:]
    grads = []
    for parcel, cut in zip(PARCELS, FAR_CUTS):
        grads.append([refs.pop(0) for _ in range(5 if cut < len(parcel) else 4)] + [None])
        grads[-1] = grads[-1][:5]
    core, shift, z_index = place_ref[0], place_ref[1], place_ref[2]
    half = own_ref.shape[1]
    tok = lhs_ref.shape[2]
    rows = 7 * tok // 2
    cut = r2a.shape[0]

    def packed(d, start, count):
        if d != 2:
            return (r0, r1, None, r3)[d][start : start + count, :]
        if start + count <= cut:
            return r2a[start : start + count, :]
        if start >= cut:
            return r2b[start - cut : start - cut + count, :]
        return jnp.concatenate([r2a[start:, :], r2b[: start + count - cut, :]], axis=0)

    for d in range(Y):
        slot = lax.rem(d - shift + Y, Y)
        for s in range(SEQS):
            for j in range(3):
                lhs_ref[s, slot, :, LANES * j : LANES * (j + 1)] = packed(
                    d, rows * s + tok * j, tok
                )
            last = packed(d, rows * s + tok * 3, tok // 2)
            lhs_ref[s, slot, : tok // 2, 3 * LANES :] = last[:, : LANES // 2]
            lhs_ref[s, slot, tok // 2 :, 3 * LANES :] = last[:, LANES // 2 :]

    spots = [(p, i) for p, parcel in enumerate(PARCELS) for i in range(len(parcel))]

    def piece(k, at, s):
        p, i = spots[at]
        whole, after, before, far_first, far_last = grads[p]
        if k != 2:
            return (whole, after, None, before)[k][i, s]
        cut = FAR_CUTS[p]
        return far_first[i, s] if i < cut else far_last[i - cut, s]

    distances = [distance for parcel in PARCELS for distance in parcel]
    for s in range(SEQS):
        lhs = lhs_ref[s].reshape(Y * tok, 2 * half)
        for i in range(0, Z, 2):
            rhs = jnp.concatenate(
                [
                    jnp.concatenate([piece(k, i, s), piece(k, i + 1, s)], axis=1)
                    for k in range(X)
                ],
                axis=0,
            )
            both = lax.dot_general(
                lhs, rhs, (((0,), (0,)), ((), ())), preferred_element_type=jnp.float32
            )
            for at in range(2):
                column = lax.rem(z_index + distances[i + at] + Z, Z)
                columns = pl.ds(pl.multiple_of(column * LANES, LANES), LANES)
                low = both[:half, LANES * at : LANES * (at + 1)]
                high = both[half:, LANES * at : LANES * (at + 1)]
                own_ref[s, :, columns] = jnp.where(core == 0, low, high)
                other_ref[s, :, columns] = jnp.where(core == 0, high, low).astype(jnp.bfloat16)


def fisher_kernel(scale, own_ref, got_ref, out_ref):
    total = None
    for s in range(SEQS):
        value = own_ref[s] + got_ref[s].astype(jnp.float32)
        total = value * value if total is None else total + value * value
    out_ref[...] = total * scale


def exchange(array):
    return lax.all_to_all(
        array, "tensor", split_axis=0, concat_axis=0, tiled=True, axis_index_groups=XZ_GROUPS
    )


def on_device(hidden_acts, out_grads):
    seq_count, tok_rows, local_ff = hidden_acts.shape
    half = tok_rows // C
    width = C * local_ff
    features = Z * C * out_grads.shape[2]
    tensor_index = lax.axis_index("tensor")
    core = tensor_index % C
    z_index = tensor_index // C % Z
    x_index = tensor_index // (Z * C)
    y_index = lax.axis_index("dp")
    places = jnp.stack([core, (x_index - y_index + Y) % Y, z_index]).astype(jnp.int32)
    first = core == 0

    low, high = out_grads[:, :half], out_grads[:, half:]
    mine, other = jnp.where(first, low, high), jnp.where(first, high, low)
    got = lax.ppermute(other, "tensor", CORE_SWAP)
    piece = jnp.concatenate([jnp.where(first, mine, got), jnp.where(first, got, mine)], axis=2)
    piece = lax.ppermute(piece, ("dp", "tensor"), XY_SWAP)

    other = lax.dynamic_slice_in_dim(hidden_acts, (1 - core) * half, half, axis=1)
    got = lax.ppermute(other, "tensor", CORE_SWAP)
    local_rot = np.kron(sylvester(local_ff // FACTOR_A), paley_matrix())
    chip_rot = np.stack([np.hstack([local_rot, local_rot]), np.hstack([local_rot, -local_rot])])
    inner = call(
        chip_rotation_kernel,
        jax.ShapeDtypeStruct((MIXED * SHARE, LANES), jnp.bfloat16),
        [SMEM, VMEM, VMEM, VMEM],
        2 * seq_count * half * width * width,
        16,
    )(places, hidden_acts, got, jnp.asarray(chip_rot, jnp.bfloat16))
    inner = exchange(inner.reshape(MIXED, SHARE, LANES))
    mixed = call(
        lambda *refs: mix_kernel(1.0 / math.sqrt(FF), *refs),
        jax.ShapeDtypeStruct((MIXED, SHARE, LANES), jnp.bfloat16),
        [VMEM],
        10**8,
        16,
        [pltpu.VMEM((MIXED, 16, LANES), jnp.float32)],
    )(inner)
    rotated = exchange(mixed).reshape(MIXED * SHARE, LANES)

    below = lax.ppermute(rotated, "dp", Y_UP)
    above = lax.ppermute(rotated, "dp", Y_DOWN)
    cut = MIXED * SHARE // 2
    far_low = lax.ppermute(below[:cut], "dp", Y_UP)
    far_high = lax.ppermute(above[cut:], "dp", Y_DOWN)

    down1 = lax.ppermute(piece, "tensor", Z_UP)
    up1 = lax.ppermute(piece, "tensor", Z_DOWN)
    down23 = lax.ppermute(jnp.stack([piece, down1]), "tensor", Z_UP2)
    up23 = lax.ppermute(jnp.stack([piece, up1]), "tensor", Z_DOWN2)
    down4 = lax.ppermute(down23[1:], "tensor", Z_UP)

    grads = []

    def along_x(block, cut):
        before = lax.ppermute(block, "tensor", X_UP)
        after = lax.ppermute(block, "tensor", X_DOWN)
        grads.extend([block, after, before])
        grads.append(lax.ppermute(before[:cut], "tensor", X_UP))
        if cut < block.shape[0]:
            grads.append(lax.ppermute(after[cut:], "tensor", X_DOWN))

    along_x(jnp.stack([piece, down1, up1]), FAR_CUTS[0])
    along_x(jnp.concatenate([down23, up23]), FAR_CUTS[1])
    along_x(down4, FAR_CUTS[2])
    own, sent = call(
        partial_kernel,
        (
            jax.ShapeDtypeStruct((seq_count, local_ff, features), jnp.float32),
            jax.ShapeDtypeStruct((seq_count, local_ff, features), jnp.bfloat16),
        ),
        [SMEM] + [VMEM] * (5 + len(grads)),
        2 * seq_count * half * Y * width * features,
        40,
        [pltpu.VMEM((seq_count, Y, half, width), jnp.bfloat16)],
    )(places, rotated, above, far_low, far_high, below, *grads)
    got = lax.ppermute(sent, "tensor", CORE_SWAP)
    return call(
        lambda *refs: fisher_kernel(1.0 / (tok_rows * Y * SEQS), *refs),
        jax.ShapeDtypeStruct((local_ff, features), jnp.float32),
        [VMEM, VMEM],
        10**7,
        16,
    )(own, got)


def solution(mesh):
    placed = (P(None, "dp", "tensor"), P(None, "dp", "tensor"))

    return jax.shard_map(
        on_device, mesh=mesh, in_specs=placed, out_specs=P("tensor", "dp"), check_vma=False
    )
```

```python
import math

import jax
import jax.numpy as jnp
import numpy as np
from jax import lax
from jax.experimental import pallas as pl
from jax.experimental.pallas import tpu as pltpu
from jax.sharding import PartitionSpec as P


FF = 14336
FACTOR_A = 28
SEQS = 3
X, Z, C, Y = 4, 8, 2, 4
LANES = 128
MIXED = X * Z
SHARE = 80


def sylvester(order):
    result = np.ones((1, 1))
    for _ in range(order.bit_length() - 1):
        result = np.kron(result, np.array([[1.0, 1.0], [1.0, -1.0]]))
    return result


def paley_matrix():
    residues = set((number * number % 13 for number in range(1, 13)))
    core_table = np.zeros((14, 14))
    core_table[0, 1:] = 1.0
    core_table[1:, 0] = 1.0
    for row_index in range(13):
        for col_index in range(13):
            offset = (col_index - row_index) % 13
            if offset != 0:
                core_table[1 + row_index, 1 + col_index] = 1.0 if offset in residues else -1.0
    return np.kron(core_table, np.array([[1.0, 1.0], [1.0, -1.0]])) + np.kron(
        np.eye(14), np.array([[1.0, -1.0], [-1.0, -1.0]])
    )


def place(x, z, c):
    return (x % X) * Z * C + (z % Z) * C + c


def pairs_of(target):
    return [
        (place(x, z, c), place(*target(x, z, c)))
        for x in range(X)
        for z in range(Z)
        for c in range(C)
    ]


CORE_SWAP = pairs_of(lambda x, z, c: (x, z, 1 - c))
X_UP = pairs_of(lambda x, z, c: (x + 1, z, c))
X_DOWN = pairs_of(lambda x, z, c: (x - 1, z, c))
X_FAR = pairs_of(lambda x, z, c: (x + 2, z, c))
Z_UP = pairs_of(lambda x, z, c: (x, z + 1, c))
Z_DOWN = pairs_of(lambda x, z, c: (x, z - 1, c))
Y_UP = [(y, (y + 1) % Y) for y in range(Y)]
Y_DOWN = [(y, (y - 1) % Y) for y in range(Y)]
XY_SWAP = [
    (y * X * Z * C + place(x, z, c), x * X * Z * C + place(y, z, c))
    for y in range(Y)
    for x in range(X)
    for z in range(Z)
    for c in range(C)
]
XZ_GROUPS = [[place(x, z, c) for x in range(X) for z in range(Z)] for c in range(C)]
DISTANCES = (0, -1, 1, -2, 2, -3, 3, 4)
VMEM = pl.BlockSpec(memory_space=pltpu.VMEM)
SMEM = pl.BlockSpec(memory_space=pltpu.SMEM)


def call(kernel, out_shape, in_specs, flops, limit_mib, scratch=()):
    many = isinstance(out_shape, tuple)
    return pl.pallas_call(
        kernel,
        out_shape=out_shape,
        in_specs=in_specs,
        out_specs=(VMEM,) * len(out_shape) if many else VMEM,
        scratch_shapes=list(scratch),
        cost_estimate=pl.CostEstimate(flops=flops, bytes_accessed=2**20, transcendentals=0),
        compiler_params=pltpu.CompilerParams(vmem_limit_bytes=limit_mib * 2**20),
    )


def chip_rotation_kernel(place_ref, acts_ref, got_ref, rot_ref, out_ref):
    core = place_ref[0]
    half = got_ref.shape[1]
    rows = 7 * half // 2
    start = pl.multiple_of(core * half, half)
    for s in range(SEQS):
        inner = jnp.dot(
            acts_ref[s, pl.ds(start, half), :], rot_ref[core], preferred_element_type=jnp.float32
        ) + jnp.dot(got_ref[s], rot_ref[1 - core], preferred_element_type=jnp.float32)
        inner = inner.astype(jnp.bfloat16)
        for j in range(3):
            out_ref[rows * s + half * j : rows * s + half * (j + 1), :] = inner[
                :, LANES * j : LANES * (j + 1)
            ]
        out_ref[rows * s + half * 3 : rows * (s + 1), :] = jnp.concatenate(
            [inner[: half // 2, 3 * LANES :], inner[half // 2 :, 3 * LANES :]], axis=1
        )
    out_ref[rows * SEQS :, :] = jnp.zeros((MIXED * SHARE - rows * SEQS, LANES), jnp.bfloat16)


def butterfly(values):
    values = list(values)
    step = 1
    while step < len(values):
        for low in range(len(values)):
            if not low & step:
                a, b = values[low], values[low | step]
                values[low], values[low | step] = a + b, a - b
        step *= 2
    return values


def mix_kernel(scale, in_ref, out_ref, mid_ref):
    for r in range(0, SHARE, 16):
        rows = slice(r, r + 16)
        for x in range(X):
            mixed = butterfly([in_ref[x * Z + z, rows, :].astype(jnp.float32) for z in range(Z)])
            for z in range(Z):
                mid_ref[x * Z + z] = mixed[z]
        for z in range(Z):
            mixed = butterfly([mid_ref[x * Z + z] for x in range(X)])
            for x in range(X):
                out_ref[x * Z + z, rows, :] = (mixed[x] * scale).astype(jnp.bfloat16)


def partial_kernel(table, place_ref, r0, r1, r2a, r2b, r3, *refs):
    grads, (own_ref, other_ref, lhs_ref) = refs[:-3], refs[-3:]
    core, shift, z_index = place_ref[0], place_ref[1], place_ref[2]
    half = own_ref.shape[1]
    tok = lhs_ref.shape[2]
    rows = 7 * tok // 2
    cut = r2a.shape[0]

    def packed(d, start, count):
        if d != 2:
            return (r0, r1, None, r3)[d][start : start + count, :]
        if start + count <= cut:
            return r2a[start : start + count, :]
        if start >= cut:
            return r2b[start - cut : start - cut + count, :]
        return jnp.concatenate([r2a[start:, :], r2b[: start + count - cut, :]], axis=0)

    for d in range(Y):
        slot = lax.rem(d - shift + Y, Y)
        for s in range(SEQS):
            for j in range(3):
                lhs_ref[s, slot, :, LANES * j : LANES * (j + 1)] = packed(
                    d, rows * s + tok * j, tok
                )
            last = packed(d, rows * s + tok * 3, tok // 2)
            lhs_ref[s, slot, : tok // 2, 3 * LANES :] = last[:, : LANES // 2]
            lhs_ref[s, slot, tok // 2 :, 3 * LANES :] = last[:, LANES // 2 :]

    def piece(k, at, s):
        array, index = table[DISTANCES[at]][k]
        return grads[array][index, s]

    for s in range(SEQS):
        lhs = lhs_ref[s].reshape(Y * tok, 2 * half)
        for i in range(0, Z, 2):
            rhs = jnp.concatenate(
                [
                    jnp.concatenate([piece(k, i, s), piece(k, i + 1, s)], axis=1)
                    for k in range(X)
                ],
                axis=0,
            )
            both = lax.dot_general(
                lhs, rhs, (((0,), (0,)), ((), ())), preferred_element_type=jnp.float32
            )
            for at in range(2):
                column = lax.rem(z_index + DISTANCES[i + at] + Z, Z)
                columns = pl.ds(pl.multiple_of(column * LANES, LANES), LANES)
                low = both[:half, LANES * at : LANES * (at + 1)]
                high = both[half:, LANES * at : LANES * (at + 1)]
                own_ref[s, :, columns] = jnp.where(core == 0, low, high)
                other_ref[s, :, columns] = jnp.where(core == 0, high, low).astype(jnp.bfloat16)


def fisher_kernel(scale, own_ref, got_ref, out_ref):
    total = None
    for s in range(SEQS):
        value = own_ref[s] + got_ref[s].astype(jnp.float32)
        total = value * value if total is None else total + value * value
    out_ref[...] = total * scale


def exchange(array):
    return lax.all_to_all(
        array, "tensor", split_axis=0, concat_axis=0, tiled=True, axis_index_groups=XZ_GROUPS
    )


def on_device(hidden_acts, out_grads):
    seq_count, tok_rows, local_ff = hidden_acts.shape
    half = tok_rows // C
    width = C * local_ff
    features = Z * C * out_grads.shape[2]
    tensor_index = lax.axis_index("tensor")
    core = tensor_index % C
    z_index = tensor_index // C % Z
    x_index = tensor_index // (Z * C)
    y_index = lax.axis_index("dp")
    places = jnp.stack([core, (x_index - y_index + Y) % Y, z_index]).astype(jnp.int32)
    first = core == 0

    low, high = out_grads[:, :half], out_grads[:, half:]
    mine, other = jnp.where(first, low, high), jnp.where(first, high, low)
    got = lax.ppermute(other, "tensor", CORE_SWAP)
    piece = jnp.concatenate([jnp.where(first, mine, got), jnp.where(first, got, mine)], axis=2)
    piece = lax.ppermute(piece, ("dp", "tensor"), XY_SWAP)

    other = lax.dynamic_slice_in_dim(hidden_acts, (1 - core) * half, half, axis=1)
    got = lax.ppermute(other, "tensor", CORE_SWAP)
    local_rot = np.kron(sylvester(local_ff // FACTOR_A), paley_matrix())
    chip_rot = np.stack([np.hstack([local_rot, local_rot]), np.hstack([local_rot, -local_rot])])
    inner = call(
        chip_rotation_kernel,
        jax.ShapeDtypeStruct((MIXED * SHARE, LANES), jnp.bfloat16),
        [SMEM, VMEM, VMEM, VMEM],
        2 * seq_count * half * width * width,
        16,
    )(places, hidden_acts, got, jnp.asarray(chip_rot, jnp.bfloat16))
    inner = exchange(inner.reshape(MIXED, SHARE, LANES))
    mixed = call(
        lambda *refs: mix_kernel(1.0 / math.sqrt(FF), *refs),
        jax.ShapeDtypeStruct((MIXED, SHARE, LANES), jnp.bfloat16),
        [VMEM],
        10**8,
        16,
        [pltpu.VMEM((MIXED, 16, LANES), jnp.float32)],
    )(inner)
    rotated = exchange(mixed).reshape(MIXED * SHARE, LANES)

    below = lax.ppermute(rotated, "dp", Y_UP)
    above = lax.ppermute(rotated, "dp", Y_DOWN)
    cut = MIXED * SHARE // 2
    far_low = lax.ppermute(below[:cut], "dp", Y_UP)
    far_high = lax.ppermute(above[cut:], "dp", Y_DOWN)

    down1 = lax.ppermute(piece, "tensor", Z_UP)
    up1 = lax.ppermute(piece, "tensor", Z_DOWN)
    down2 = lax.ppermute(down1, "tensor", Z_UP)
    up2 = lax.ppermute(up1, "tensor", Z_DOWN)
    down3 = lax.ppermute(down2, "tensor", Z_UP)
    up3 = lax.ppermute(up2, "tensor", Z_DOWN)
    down4 = lax.ppermute(down3, "tensor", Z_UP)

    grads, table = [], {}

    def keep(array):
        grads.append(array)
        return len(grads) - 1

    def along_x(block, distances, cut):
        before = lax.ppermute(block, "tensor", X_UP)
        after = lax.ppermute(block, "tensor", X_DOWN)
        fars = []
        if cut:
            far = lax.ppermute(before[:cut], "tensor", X_UP)
            fars += [(keep(far), i) for i in range(cut)]
        if cut is None:
            far = keep(lax.ppermute(block, "tensor", X_FAR))
            fars = [(far, i) for i in range(len(distances))]
        elif cut < len(distances):
            far = lax.ppermute(after[cut:], "tensor", X_DOWN)
            fars += [(keep(far), i) for i in range(len(distances) - cut)]
        spots = keep(block), keep(after), keep(before)
        for i, distance in enumerate(distances):
            table[distance] = ((spots[0], i), (spots[1], i), fars[i], (spots[2], i))

    along_x(piece[None], (0,), 1)
    others = jnp.concatenate([grads[array] for array, index in table[0][1:]])
    for distance, near, pairs in ((-1, down1, Z_UP), (1, up1, Z_DOWN)):
        rest = keep(lax.ppermute(others, "tensor", pairs))
        table[distance] = ((keep(near[None]), 0), (rest, 0), (rest, 1), (rest, 2))
    along_x(jnp.stack([down2, up2]), (-2, 2), 1)
    along_x(jnp.stack([down3, up3]), (-3, 3), 1)
    along_x(down4[None], (4,), None)
    own, sent = call(
        lambda *refs: partial_kernel(table, *refs),
        (
            jax.ShapeDtypeStruct((seq_count, local_ff, features), jnp.float32),
            jax.ShapeDtypeStruct((seq_count, local_ff, features), jnp.bfloat16),
        ),
        [SMEM] + [VMEM] * (5 + len(grads)),
        2 * seq_count * half * Y * width * features,
        40,
        [pltpu.VMEM((seq_count, Y, half, width), jnp.bfloat16)],
    )(places, rotated, above, far_low, far_high, below, *grads)
    got = lax.ppermute(sent, "tensor", CORE_SWAP)
    return call(
        lambda *refs: fisher_kernel(1.0 / (tok_rows * Y * SEQS), *refs),
        jax.ShapeDtypeStruct((local_ff, features), jnp.float32),
        [VMEM, VMEM],
        10**7,
        16,
    )(own, got)


def solution(mesh):
    placed = (P(None, "dp", "tensor"), P(None, "dp", "tensor"))

    return jax.shard_map(
        on_device, mesh=mesh, in_specs=placed, out_specs=P("tensor", "dp"), check_vma=False
    )
```

```python
import math

import jax
import jax.numpy as jnp
import numpy as np
from jax import lax
from jax.experimental import pallas as pl
from jax.experimental.pallas import tpu as pltpu
from jax.sharding import PartitionSpec as P


FF = 14336
FACTOR_A = 28
SEQS = 3
X, Z, C, Y = 4, 8, 2, 4
LANES = 128
MIXED = X * Z
SHARE = 80


def sylvester(order):
    result = np.ones((1, 1))
    for _ in range(order.bit_length() - 1):
        result = np.kron(result, np.array([[1.0, 1.0], [1.0, -1.0]]))
    return result


def paley_matrix():
    residues = set((number * number % 13 for number in range(1, 13)))
    core_table = np.zeros((14, 14))
    core_table[0, 1:] = 1.0
    core_table[1:, 0] = 1.0
    for row_index in range(13):
        for col_index in range(13):
            offset = (col_index - row_index) % 13
            if offset != 0:
                core_table[1 + row_index, 1 + col_index] = 1.0 if offset in residues else -1.0
    return np.kron(core_table, np.array([[1.0, 1.0], [1.0, -1.0]])) + np.kron(
        np.eye(14), np.array([[1.0, -1.0], [-1.0, -1.0]])
    )


def place(x, z, c):
    return (x % X) * Z * C + (z % Z) * C + c


def pairs_of(target):
    return [
        (place(x, z, c), place(*target(x, z, c)))
        for x in range(X)
        for z in range(Z)
        for c in range(C)
    ]


CORE_SWAP = pairs_of(lambda x, z, c: (x, z, 1 - c))
X_UP = pairs_of(lambda x, z, c: (x + 1, z, c))
X_DOWN = pairs_of(lambda x, z, c: (x - 1, z, c))
X_FAR = pairs_of(lambda x, z, c: (x + 2, z, c))
Z_UP = pairs_of(lambda x, z, c: (x, z + 1, c))
Z_DOWN = pairs_of(lambda x, z, c: (x, z - 1, c))
Y_UP = [(y, (y + 1) % Y) for y in range(Y)]
Y_DOWN = [(y, (y - 1) % Y) for y in range(Y)]
XY_SWAP = [
    (y * X * Z * C + place(x, z, c), x * X * Z * C + place(y, z, c))
    for y in range(Y)
    for x in range(X)
    for z in range(Z)
    for c in range(C)
]
XZ_GROUPS = [[place(x, z, c) for x in range(X) for z in range(Z)] for c in range(C)]
DISTANCES = (0, -1, 1, -2, 2, -3, 3, 4)
VMEM = pl.BlockSpec(memory_space=pltpu.VMEM)
SMEM = pl.BlockSpec(memory_space=pltpu.SMEM)


def call(kernel, out_shape, in_specs, flops, limit_mib, scratch=()):
    many = isinstance(out_shape, tuple)
    return pl.pallas_call(
        kernel,
        out_shape=out_shape,
        in_specs=in_specs,
        out_specs=(VMEM,) * len(out_shape) if many else VMEM,
        scratch_shapes=list(scratch),
        cost_estimate=pl.CostEstimate(flops=flops, bytes_accessed=2**20, transcendentals=0),
        compiler_params=pltpu.CompilerParams(vmem_limit_bytes=limit_mib * 2**20),
    )


def chip_rotation_kernel(place_ref, acts_ref, got_ref, rot_ref, out_ref):
    core = place_ref[0]
    half = got_ref.shape[1]
    rows = 7 * half // 2
    start = pl.multiple_of(core * half, half)
    for s in range(SEQS):
        inner = jnp.dot(
            acts_ref[s, pl.ds(start, half), :], rot_ref[core], preferred_element_type=jnp.float32
        ) + jnp.dot(got_ref[s], rot_ref[1 - core], preferred_element_type=jnp.float32)
        inner = inner.astype(jnp.bfloat16)
        for j in range(3):
            out_ref[rows * s + half * j : rows * s + half * (j + 1), :] = inner[
                :, LANES * j : LANES * (j + 1)
            ]
        out_ref[rows * s + half * 3 : rows * (s + 1), :] = jnp.concatenate(
            [inner[: half // 2, 3 * LANES :], inner[half // 2 :, 3 * LANES :]], axis=1
        )
    out_ref[rows * SEQS :, :] = jnp.zeros((MIXED * SHARE - rows * SEQS, LANES), jnp.bfloat16)


def butterfly(values):
    values = list(values)
    step = 1
    while step < len(values):
        for low in range(len(values)):
            if not low & step:
                a, b = values[low], values[low | step]
                values[low], values[low | step] = a + b, a - b
        step *= 2
    return values


def mix_kernel(scale, in_ref, out_ref, mid_ref):
    for r in range(0, SHARE, 16):
        rows = slice(r, r + 16)
        for x in range(X):
            mixed = butterfly([in_ref[x * Z + z, rows, :].astype(jnp.float32) for z in range(Z)])
            for z in range(Z):
                mid_ref[x * Z + z] = mixed[z]
        for z in range(Z):
            mixed = butterfly([mid_ref[x * Z + z] for x in range(X)])
            for x in range(X):
                out_ref[x * Z + z, rows, :] = (mixed[x] * scale).astype(jnp.bfloat16)


def unpack(packed, store):
    tok = 224
    rows = 7 * tok // 2
    for s in range(SEQS):
        for j in range(3):
            columns = slice(LANES * j, LANES * (j + 1))
            store(s, slice(0, tok), columns, packed(rows * s + tok * j, tok))
        last = packed(rows * s + tok * 3, tok // 2)
        columns = slice(3 * LANES, 3 * LANES + LANES // 2)
        store(s, slice(0, tok // 2), columns, last[:, : LANES // 2])
        store(s, slice(tok // 2, tok), columns, last[:, LANES // 2 :])


def unpack_kernel(place_ref, r0, r1, r3, lhs_ref):
    for d, ref in ((0, r0), (1, r1), (3, r3)):
        slot = lax.rem(d - place_ref[1] + Y, Y)

        def store(s, rows, columns, value):
            lhs_ref[s, slot, rows, columns] = value

        unpack(lambda start, count: ref[start : start + count, :], store)


def partial_kernel(table, place_ref, early_ref, r2a, r2b, *refs):
    grads, (own_ref, other_ref, far_ref) = refs[:-3], refs[-3:]
    core, shift, z_index = place_ref[0], place_ref[1], place_ref[2]
    half = own_ref.shape[1]
    cut = r2a.shape[0]
    far_slot = lax.rem(2 - shift + Y, Y)

    def packed(start, count):
        if start + count <= cut:
            return r2a[start : start + count, :]
        if start >= cut:
            return r2b[start - cut : start - cut + count, :]
        return jnp.concatenate([r2a[start:, :], r2b[: start + count - cut, :]], axis=0)

    def store(s, rows, columns, value):
        far_ref[s, rows, columns] = value

    unpack(packed, store)

    def piece(k, at, s):
        array, index = table[DISTANCES[at]][k]
        return grads[array][index, s]

    for s in range(SEQS):
        lhs = jnp.concatenate(
            [jnp.where(far_slot == k, far_ref[s], early_ref[s, k]) for k in range(Y)], axis=0
        )
        for i in range(0, Z, 2):
            rhs = jnp.concatenate(
                [
                    jnp.concatenate([piece(k, i, s), piece(k, i + 1, s)], axis=1)
                    for k in range(X)
                ],
                axis=0,
            )
            both = lax.dot_general(
                lhs, rhs, (((0,), (0,)), ((), ())), preferred_element_type=jnp.float32
            )
            for at in range(2):
                column = lax.rem(z_index + DISTANCES[i + at] + Z, Z)
                columns = pl.ds(pl.multiple_of(column * LANES, LANES), LANES)
                low = both[:half, LANES * at : LANES * (at + 1)]
                high = both[half:, LANES * at : LANES * (at + 1)]
                own_ref[s, :, columns] = jnp.where(core == 0, low, high)
                other_ref[s, :, columns] = jnp.where(core == 0, high, low).astype(jnp.bfloat16)


def fisher_kernel(scale, own_ref, got_ref, out_ref):
    total = None
    for s in range(SEQS):
        value = own_ref[s] + got_ref[s].astype(jnp.float32)
        total = value * value if total is None else total + value * value
    out_ref[...] = total * scale


def exchange(array):
    return lax.all_to_all(
        array, "tensor", split_axis=0, concat_axis=0, tiled=True, axis_index_groups=XZ_GROUPS
    )


def on_device(hidden_acts, out_grads):
    seq_count, tok_rows, local_ff = hidden_acts.shape
    half = tok_rows // C
    width = C * local_ff
    features = Z * C * out_grads.shape[2]
    tensor_index = lax.axis_index("tensor")
    core = tensor_index % C
    z_index = tensor_index // C % Z
    x_index = tensor_index // (Z * C)
    y_index = lax.axis_index("dp")
    places = jnp.stack([core, (x_index - y_index + Y) % Y, z_index]).astype(jnp.int32)
    first = core == 0

    low, high = out_grads[:, :half], out_grads[:, half:]
    mine, other = jnp.where(first, low, high), jnp.where(first, high, low)
    got = lax.ppermute(other, "tensor", CORE_SWAP)
    piece = jnp.concatenate([jnp.where(first, mine, got), jnp.where(first, got, mine)], axis=2)
    piece = lax.ppermute(piece, ("dp", "tensor"), XY_SWAP)

    other = lax.dynamic_slice_in_dim(hidden_acts, (1 - core) * half, half, axis=1)
    got = lax.ppermute(other, "tensor", CORE_SWAP)
    local_rot = np.kron(sylvester(local_ff // FACTOR_A), paley_matrix())
    chip_rot = np.stack([np.hstack([local_rot, local_rot]), np.hstack([local_rot, -local_rot])])
    inner = call(
        chip_rotation_kernel,
        jax.ShapeDtypeStruct((MIXED * SHARE, LANES), jnp.bfloat16),
        [SMEM, VMEM, VMEM, VMEM],
        2 * seq_count * half * width * width,
        16,
    )(places, hidden_acts, got, jnp.asarray(chip_rot, jnp.bfloat16))
    inner = exchange(inner.reshape(MIXED, SHARE, LANES))
    mixed = call(
        lambda *refs: mix_kernel(1.0 / math.sqrt(FF), *refs),
        jax.ShapeDtypeStruct((MIXED, SHARE, LANES), jnp.bfloat16),
        [VMEM],
        10**8,
        16,
        [pltpu.VMEM((MIXED, 16, LANES), jnp.float32)],
    )(inner)
    rotated = exchange(mixed).reshape(MIXED * SHARE, LANES)

    below = lax.ppermute(rotated, "dp", Y_UP)
    above = lax.ppermute(rotated, "dp", Y_DOWN)
    cut = MIXED * SHARE // 2
    far_low = lax.ppermute(below[:cut], "dp", Y_UP)
    far_high = lax.ppermute(above[cut:], "dp", Y_DOWN)

    down1 = lax.ppermute(piece, "tensor", Z_UP)
    up1 = lax.ppermute(piece, "tensor", Z_DOWN)
    down2 = lax.ppermute(down1, "tensor", Z_UP)
    up2 = lax.ppermute(up1, "tensor", Z_DOWN)
    down3 = lax.ppermute(down2, "tensor", Z_UP)
    up3 = lax.ppermute(up2, "tensor", Z_DOWN)
    down4 = lax.ppermute(down3, "tensor", Z_UP)

    grads, table = [], {}

    def keep(array):
        grads.append(array)
        return len(grads) - 1

    def along_x(block, distances, cut):
        before = lax.ppermute(block, "tensor", X_UP)
        after = lax.ppermute(block, "tensor", X_DOWN)
        fars = []
        if cut:
            far = lax.ppermute(before[:cut], "tensor", X_UP)
            fars += [(keep(far), i) for i in range(cut)]
        if cut is None:
            far = keep(lax.ppermute(block, "tensor", X_FAR))
            fars = [(far, i) for i in range(len(distances))]
        elif cut < len(distances):
            far = lax.ppermute(after[cut:], "tensor", X_DOWN)
            fars += [(keep(far), i) for i in range(len(distances) - cut)]
        spots = keep(block), keep(after), keep(before)
        for i, distance in enumerate(distances):
            table[distance] = ((spots[0], i), (spots[1], i), fars[i], (spots[2], i))

    along_x(piece[None], (0,), 1)
    others = jnp.concatenate([grads[array] for array, index in table[0][1:]])
    for distance, near, pairs in ((-1, down1, Z_UP), (1, up1, Z_DOWN)):
        rest = keep(lax.ppermute(others, "tensor", pairs))
        table[distance] = ((keep(near[None]), 0), (rest, 0), (rest, 1), (rest, 2))
    along_x(jnp.stack([down2, up2]), (-2, 2), 1)
    along_x(jnp.stack([down3, up3]), (-3, 3), 1)
    along_x(down4[None], (4,), None)
    early = call(
        unpack_kernel,
        jax.ShapeDtypeStruct((seq_count, Y, half, width), jnp.bfloat16),
        [SMEM, VMEM, VMEM, VMEM],
        10**7,
        16,
    )(places, rotated, above, below)
    own, sent = call(
        lambda *refs: partial_kernel(table, *refs),
        (
            jax.ShapeDtypeStruct((seq_count, local_ff, features), jnp.float32),
            jax.ShapeDtypeStruct((seq_count, local_ff, features), jnp.bfloat16),
        ),
        [SMEM] + [VMEM] * (3 + len(grads)),
        2 * seq_count * half * Y * width * features,
        40,
        [pltpu.VMEM((seq_count, half, width), jnp.bfloat16)],
    )(places, early, far_low, far_high, *grads)
    got = lax.ppermute(sent, "tensor", CORE_SWAP)
    return call(
        lambda *refs: fisher_kernel(1.0 / (tok_rows * Y * SEQS), *refs),
        jax.ShapeDtypeStruct((local_ff, features), jnp.float32),
        [VMEM, VMEM],
        10**7,
        16,
    )(own, got)


def solution(mesh):
    placed = (P(None, "dp", "tensor"), P(None, "dp", "tensor"))

    return jax.shard_map(
        on_device, mesh=mesh, in_specs=placed, out_specs=P("tensor", "dp"), check_vma=False
    )
```
